32 devices in a mesh: data: 2 (over x), dap2: 4 (over z), dap: 4 (over y, core).
Axes of the slice: x: 2, y: 2, z: 4, core: 2. Of those that a mesh axis runs over, the one named last changes fastest.
Arguments:
- pair_act: bfloat16 [768, 384, 128], P(('data', 'dap'), 'dap2'), parts along dimension 0
- pair_mask: int32 [768, 384], P(('data', 'dap'), 'dap2'), parts along dimension 0
- in_gamma: float32 [4, 2, 128], replicated
- in_beta: float32 [4, 2, 128], replicated
- w_proj: bfloat16 [4, 2, 128, 512], replicated
- w_gate: bfloat16 [4, 2, 128, 128], replicated
- out_gamma: float32 [4, 2, 128], replicated
- out_beta: float32 [4, 2, 128], replicated
- w_out: bfloat16 [4, 2, 128, 128], replicated
Outputs:
- output: bfloat16 [768, 384, 128], P(('data', 'dap'), 'dap2'), parts along dimension 0
There are 2 independent parts. The reference program is written for one: setup_inputs(seed, part) draws one part's arguments, and reference() takes and returns one part's arrays. A program takes and returns all parts, laid end to end along the dimension named above; an argument that names none is the same for every part.
All inputs are finite; a program needn't handle non-finite values.
Results may differ from the reference program's by a relative error of at most 0.0146083.
Values are sent between devices in bfloat16 or wider.
A program may use at most 1 GiB of HBM per device.

```python
import jax
import jax.numpy as jnp
from jax import lax

RESIDUES = 384
PAIR_DIM = 128
TRI_DIM = 128
BLOCKS = 4
NORM_EPS = 1e-5


def setup_inputs(seed: int = 0, part: int = 0) -> dict:
    key_list = jax.random.split(jax.random.key(seed), 9)
    pair_key = jax.random.fold_in(key_list[0], part)
    mask_key = jax.random.fold_in(key_list[1], part)
    pair_act = jax.random.normal(pair_key, (RESIDUES, RESIDUES, PAIR_DIM), jnp.float32).astype(jnp.bfloat16)
    row_valid = (jax.random.randint(mask_key, (RESIDUES,), 0, 16) != 0).astype(jnp.int32)
    pair_mask = row_valid[:, None] * row_valid[None, :]
    stack_shape = (BLOCKS, 2)
    in_gamma = 1.0 + 0.3 * jax.random.normal(key_list[2], stack_shape + (PAIR_DIM,), jnp.float32)
    in_beta = 0.3 * jax.random.normal(key_list[3], stack_shape + (PAIR_DIM,), jnp.float32)
    w_proj = (jax.random.normal(key_list[4], stack_shape + (PAIR_DIM, 4 * TRI_DIM), jnp.float32) * PAIR_DIM ** -0.5).astype(jnp.bfloat16)
    w_gate = (jax.random.normal(key_list[5], stack_shape + (PAIR_DIM, PAIR_DIM), jnp.float32) * PAIR_DIM ** -0.5).astype(jnp.bfloat16)
    out_gamma = 1.0 + 0.3 * jax.random.normal(key_list[6], stack_shape + (TRI_DIM,), jnp.float32)
    out_beta = 0.3 * jax.random.normal(key_list[7], stack_shape + (TRI_DIM,), jnp.float32)
    w_out = (jax.random.normal(key_list[8], stack_shape + (TRI_DIM, PAIR_DIM), jnp.float32) * TRI_DIM ** -0.5).astype(jnp.bfloat16)
    return {'pair_act': pair_act, 'pair_mask': pair_mask, 'in_gamma': in_gamma, 'in_beta': in_beta, 'w_proj': w_proj, 'w_gate': w_gate, 'out_gamma': out_gamma, 'out_beta': out_beta, 'w_out': w_out}


def layer_norm(values, gamma, beta):
    centered = values - jnp.mean(values, axis=-1, keepdims=True)
    variance = jnp.mean(centered * centered, axis=-1, keepdims=True)
    return centered * lax.rsqrt(variance + NORM_EPS) * gamma + beta


def project_row(pair_row, mask_row, gamma_in, beta_in, w_proj):
    normed = layer_norm(pair_row.astype(jnp.float32), gamma_in, beta_in).astype(jnp.bfloat16)
    projected = jnp.dot(normed, w_proj, preferred_element_type=jnp.float32)
    mask_col = mask_row.astype(jnp.float32)[:, None]
    left = mask_col * jax.nn.sigmoid(projected[:, TRI_DIM:2 * TRI_DIM]) * projected[:, :TRI_DIM]
    right = mask_col * jax.nn.sigmoid(projected[:, 3 * TRI_DIM:]) * projected[:, 2 * TRI_DIM:3 * TRI_DIM]
    return left.astype(jnp.bfloat16), right.astype(jnp.bfloat16)


def finish_row(pair_row, tri_row, gamma_in, beta_in, w_gate, gamma_out, beta_out, w_out):
    normed = layer_norm(pair_row.astype(jnp.float32), gamma_in, beta_in).astype(jnp.bfloat16)
    gate = jax.nn.sigmoid(jnp.dot(normed, w_gate, preferred_element_type=jnp.float32))
    tri_normed = layer_norm(tri_row.astype(jnp.float32), gamma_out, beta_out).astype(jnp.bfloat16)
    update = jnp.dot(tri_normed, w_out, preferred_element_type=jnp.float32)
    return (pair_row.astype(jnp.float32) + gate * update).astype(jnp.bfloat16)


def triangle_update(pair_act, pair_mask, params, incoming):
    gamma_in, beta_in, w_proj, w_gate, gamma_out, beta_out, w_out = params
    left, right = lax.map(lambda rows: project_row(rows[0], rows[1], gamma_in, beta_in, w_proj), (pair_act, pair_mask))
    einsum_form = 'kic,kjc->ijc' if incoming else 'ikc,jkc->ijc'
    tri_out = jnp.einsum(einsum_form, left.astype(jnp.float32), right.astype(jnp.float32)).astype(jnp.bfloat16)
    return lax.map(lambda rows: finish_row(rows[0], rows[1], gamma_in, beta_in, w_gate, gamma_out, beta_out, w_out), (pair_act, tri_out))


def reference(pair_act, pair_mask, in_gamma, in_beta, w_proj, w_gate, out_gamma, out_beta, w_out):
    def block_step(carry, params):
        outgoing = tuple(leaf[0] for leaf in params)
        incoming = tuple(leaf[1] for leaf in params)
        carry = triangle_update(carry, pair_mask, outgoing, False)
        carry = triangle_update(carry, pair_mask, incoming, True)
        return carry, None
    result, _ = lax.scan(block_step, pair_act, (in_gamma, in_beta, w_proj, w_gate, out_gamma, out_beta, w_out))
    return result
```

```python
import functools

import jax
import jax.numpy as jnp
from jax import lax
from jax.experimental import pallas as pl
from jax.experimental.pallas import tpu as pltpu
from jax.sharding import PartitionSpec as P

NORM_EPS = 1e-5
MESH = pl.DeviceIdType.MESH
N = 384
C = 128
D = 16
ROWS = N // D
BLK = 96
CPD = C // D
CHUNK = 8
NCHUNK = ROWS // CHUNK
LT = N // 128
UPDATES = 8


def sigmoid(x):
    return 0.5 * jnp.tanh(0.5 * x) + 0.5


def norm_channels(v, gamma, beta):
    mean = jnp.sum(v, axis=0, keepdims=True) * (1.0 / C)
    centered = v - mean
    variance = jnp.sum(centered * centered, axis=0, keepdims=True) * (1.0 / C)
    return centered * lax.rsqrt(variance + NORM_EPS) * gamma + beta


def kernel(z_in, m_in, gin, bin_, wp, wg, gout, bout, wo, out,
           zrow, mrow, mask, z, gate, x, q, y, ab, r, s, t, tsend, trecv,
           zsend_sem, msend_sem, zrecv_sem, mrecv_sem, absend_sem, abrecv_sem, tsend_sem, trecv_sem,
           osend_sem, orecv_sem):
    g = lax.axis_index("data")
    jz = lax.axis_index("dap2")
    iy = lax.axis_index("dap")
    half = jz // 2
    zl = jz % 2
    me = g * 8 + zl * 4 + iy
    row0 = me * ROWS

    def place(d):
        px = (g + d // 8) % 2
        pz = (zl + (d // 4) % 2) % 2
        py = (iy + d % 4) % 4
        return (px, 2 * half + pz, py), px * 8 + pz * 4 + py

    def blocks_out(q_, start):
        here = jnp.logical_and(jnp.logical_and(iy // 2 == g, jz == 2 * g + iy % 2), iy == q_)
        dst = (iy // 2, 2 * g + iy % 2, q_)
        rows = pl.ds(q_ * ROWS, ROWS)
        cols = pl.ds(pl.multiple_of(jz * BLK, 32), BLK)
        for src, dst_ref, send, recv in (
            (z_in.at[rows], zrow.at[:, cols, :], zsend_sem.at[q_], zrecv_sem),
            (m_in.at[rows], mrow.at[jz], msend_sem.at[q_], mrecv_sem),
        ):
            @pl.when(jnp.logical_not(here))
            def _():
                copy = pltpu.make_async_remote_copy(src, dst_ref, send, recv, device_id=dst, device_id_type=MESH)
                if start:
                    copy.start()
                else:
                    copy.wait_send()

            if start:
                @pl.when(here)
                def _():
                    pltpu.make_async_copy(src, dst_ref, recv).start()

    for q_ in range(4):
        blocks_out(q_, True)
    pltpu.make_async_copy(mrow, mrow, mrecv_sem).wait()
    pltpu.make_async_copy(zrow, zrow, zrecv_sem).wait()
    lane = lax.broadcasted_iota(jnp.int32, (128, N), 0)
    col = lax.broadcasted_iota(jnp.int32, (128, N), 1)
    total = jnp.zeros((ROWS, N), jnp.float32)
    for j in range(4):
        pick = jnp.logical_and(col == lane + j * BLK, lane < BLK).astype(jnp.float32)
        total = total + jnp.dot(mrow[j], pick, preferred_element_type=jnp.float32)
    mask[...] = total
    for q_ in range(4):
        blocks_out(q_, False)

    def turn_in(i, _):
        z[i] = zrow[i].T
        return 0

    lax.fori_loop(0, ROWS, turn_in, 0)

    def project(u, p):
        for h in range(2):
            for lt in range(LT):
                v = z[2 * p + h, :, pl.ds(lt * 128, 128)].astype(jnp.float32)
                xn = norm_channels(v, gin[u], bin_[u])
                x[:, pl.ds(h * N + lt * 128, 128)] = xn.astype(jnp.bfloat16)
        q[pl.ds(0, 4 * C), :] = jnp.dot(wp[u], x[...], preferred_element_type=jnp.float32)
        q[pl.ds(4 * C, C), :] = jnp.dot(wg[u], x[...], preferred_element_type=jnp.float32)
        for h in range(2):
            cols = pl.ds(h * N, N)
            m = mask[pl.ds(2 * p + h, 1), :]
            for d in range(D):
                def part(k):
                    return q[pl.ds(k * C + d * CPD, CPD), cols]
                left = m * sigmoid(part(1)) * part(0)
                right = m * sigmoid(part(3)) * part(2)
                ab[d, 2 * p + h] = jnp.concatenate([left, right], axis=0).astype(jnp.bfloat16)
                gate[2 * p + h, pl.ds(d * CPD, CPD), :] = sigmoid(part(4))

    def finish(u, p):
        for lt in range(LT):
            tv = trecv[:, p, :, pl.ds(lt * 128, 128)].astype(jnp.float32)
            for h in range(2):
                v = tv[:, h * CPD:(h + 1) * CPD, :].reshape(C, 128)
                yn = norm_channels(v, gout[u], bout[u])
                y[:, pl.ds(h * N + lt * 128, 128)] = yn.astype(jnp.bfloat16)
        q[pl.ds(0, C), :] = jnp.dot(wo[u], y[...], preferred_element_type=jnp.float32)
        for h in range(2):
            for k in range(C // 16):
                rows = pl.ds(k * 16, 16)
                upd = gate[2 * p + h, rows, :] * q[rows, pl.ds(h * N, N)]
                z[2 * p + h, rows, :] = (z[2 * p + h, rows, :].astype(jnp.float32) + upd).astype(jnp.bfloat16)

    def send_ab(c):
        mine = pl.ds(pl.multiple_of(row0 + c * CHUNK, 8), CHUNK)
        rows = pl.ds(c * CHUNK, CHUNK)

        def to(d, _):
            dst, num = place(d)
            pltpu.make_async_remote_copy(ab.at[num, rows], r.at[mine], absend_sem, abrecv_sem.at[c],
                                         device_id=dst, device_id_type=MESH).start()
            return 0

        lax.fori_loop(1, D, to, 0)
        r[mine] = ab[me, rows]

    def project_chunk(u, c):
        def one(p, _):
            project(u, c * (CHUNK // 2) + p)
            return 0

        lax.fori_loop(0, CHUNK // 2, one, 0)
        send_ab(c)

    for c in range(NCHUNK):
        project_chunk(0, c)

    def update(u, _):
        for c in range(NCHUNK):
            part = r.at[pl.ds(0, (D - 1) * CHUNK)]
            pltpu.make_async_copy(part, part, abrecv_sem.at[c]).wait()

            def turn(k, _):
                rows = pl.ds(pl.multiple_of(k * ROWS + c * CHUNK, 8), CHUNK)
                for lt in range(LT):
                    v = r[rows, :, pl.ds(lt * 128, 128)].astype(jnp.float32)
                    s[:, lt, rows, :] = jnp.swapaxes(v, 0, 1)
                return 0

            lax.fori_loop(0, D, turn, 0)

        def square(c):
            return jnp.concatenate([s[c, lt] for lt in range(LT)], axis=1).astype(jnp.bfloat16)

        def contract(c, dims):
            prod = lax.dot_general(square(c), square(c + CPD), (dims, ((), ())), preferred_element_type=jnp.float32)
            for lt in range(LT):
                t[c, lt] = prod[:, lt * 128:(lt + 1) * 128]

        @pl.when(u % 2 == 0)
        def _():
            def one(c, _):
                contract(c, ((1,), (1,)))
                return 0
            lax.fori_loop(0, CPD, one, 0)

        @pl.when(u % 2 == 1)
        def _():
            def one(c, _):
                contract(c, ((0,), (0,)))
                return 0
            lax.fori_loop(0, CPD, one, 0)

        def give(d, _):
            dst, num = place(d)
            for k in range(NCHUNK):
                rows = pl.ds(pl.multiple_of(num * ROWS + k * 8, 8), 8)
                pairs = pl.ds(num * (ROWS // 2) + k * 4, 4)
                for lt in range(LT):
                    v = jnp.swapaxes(t[:, lt, rows, :], 0, 1)
                    tsend[pairs, :, pl.ds(lt * 128, 128)] = v.reshape(4, 16, 128).astype(jnp.bfloat16)
            pairs = pl.ds(num * (ROWS // 2), ROWS // 2)

            @pl.when(d > 0)
            def _():
                pltpu.make_async_remote_copy(tsend.at[pairs], trecv.at[me], tsend_sem, trecv_sem,
                                             device_id=dst, device_id_type=MESH).start()

            @pl.when(d == 0)
            def _():
                trecv[me] = tsend[pairs]
            return 0

        lax.fori_loop(0, D, give, 0)
        part = trecv.at[pl.ds(0, D - 1)]
        pltpu.make_async_copy(part, part, trecv_sem).wait()
        part = ab.at[pl.ds(0, D - 1)]
        pltpu.make_async_copy(part, part, absend_sem).wait()
        part = tsend.at[pl.ds(0, (D - 1) * (ROWS // 2))]
        pltpu.make_async_copy(part, part, tsend_sem).wait()

        for c in range(NCHUNK):
            def one(p, _):
                finish(u, c * (CHUNK // 2) + p)
                return 0

            lax.fori_loop(0, CHUNK // 2, one, 0)

            @pl.when(u < UPDATES - 1)
            def _():
                project_chunk(jnp.minimum(u + 1, UPDATES - 1), c)
        return 0

    lax.fori_loop(0, UPDATES, update, 0)

    def turn_out(i, _):
        zrow[i] = z[i].T
        return 0

    lax.fori_loop(0, ROWS, turn_out, 0)

    home = 2 * g + zl
    mine = pl.ds(pl.multiple_of(iy * ROWS, 8), ROWS)

    def blocks_back(j, start):
        here = jnp.logical_and(jnp.logical_and(half == g, jz == j), iy == home)
        src = zrow.at[:, pl.ds(j * BLK, BLK), :]
        dst_ref = out.at[mine]

        @pl.when(jnp.logical_not(here))
        def _():
            copy = pltpu.make_async_remote_copy(src, dst_ref, osend_sem.at[j], orecv_sem,
                                                device_id=(half, j, home), device_id_type=MESH)
            if start:
                copy.start()
            else:
                copy.wait_send()

        if start:
            @pl.when(here)
            def _():
                pltpu.make_async_copy(src, dst_ref, orecv_sem).start()

    for j in range(4):
        blocks_back(j, True)
    pltpu.make_async_copy(out, out, orecv_sem).wait()
    for j in range(4):
        blocks_back(j, False)


def local_fn(pair_act, pair_mask, in_gamma, in_beta, w_proj, w_gate, out_gamma, out_beta, w_out):
    mask = jnp.pad(pair_mask.astype(jnp.float32), ((0, 0), (0, 128 - BLK)))

    def spread(v):
        return jnp.broadcast_to(v.reshape(UPDATES, C, 1), (UPDATES, C, 128))

    def turned(w):
        return jnp.swapaxes(w.reshape((UPDATES,) + w.shape[2:]), 1, 2)

    any_spec = pl.BlockSpec(memory_space=pl.ANY)
    vmem = pl.BlockSpec(memory_space=pltpu.VMEM)
    bf16, f32 = jnp.bfloat16, jnp.float32
    return pl.pallas_call(
        kernel,
        out_shape=jax.ShapeDtypeStruct((BLK, BLK, C), bf16),
        in_specs=[any_spec, any_spec] + [vmem] * 7,
        out_specs=any_spec,
        scratch_shapes=[
            pltpu.VMEM((ROWS, N, C), bf16),
            pltpu.VMEM((4, ROWS, 128), f32),
            pltpu.VMEM((ROWS, N), f32),
            pltpu.VMEM((ROWS, C, N), bf16),
            pltpu.VMEM((ROWS, C, N), f32),
            pltpu.VMEM((C, 2 * N), bf16),
            pltpu.VMEM((5 * C, 2 * N), f32),
            pltpu.VMEM((C, 2 * N), bf16),
            pltpu.VMEM((D, ROWS, 2 * CPD, N), bf16),
            pltpu.VMEM((N, 2 * CPD, N), bf16),
            pltpu.VMEM((2 * CPD, LT, N, 128), f32),
            pltpu.VMEM((CPD, LT, N, 128), f32),
            pltpu.VMEM((N // 2, 2 * CPD, N), bf16),
            pltpu.VMEM((D, ROWS // 2, 2 * CPD, N), bf16),
            pltpu.SemaphoreType.DMA((4,)),
            pltpu.SemaphoreType.DMA((4,)),
            pltpu.SemaphoreType.DMA,
            pltpu.SemaphoreType.DMA,
            pltpu.SemaphoreType.DMA,
            pltpu.SemaphoreType.DMA((NCHUNK,)),
            pltpu.SemaphoreType.DMA,
            pltpu.SemaphoreType.DMA,
            pltpu.SemaphoreType.DMA((4,)),
            pltpu.SemaphoreType.DMA,
        ],
        compiler_params=pltpu.CompilerParams(has_side_effects=True, vmem_limit_bytes=60 * 1024 * 1024),
        name="triangle",
    )(pair_act, mask, spread(in_gamma), spread(in_beta), turned(w_proj), turned(w_gate),
      spread(out_gamma), spread(out_beta), turned(w_out))


def solution(mesh):
    pair_spec = P(("data", "dap"), "dap2", None)
    mask_spec = P(("data", "dap"), "dap2")
    return jax.shard_map(local_fn, mesh=mesh, in_specs=(pair_spec, mask_spec) + (P(),) * 7,
                         out_specs=pair_spec, check_vma=False)
```

```python
import functools

import jax
import jax.numpy as jnp
from jax import lax
from jax.experimental import pallas as pl
from jax.experimental.pallas import tpu as pltpu
from jax.sharding import PartitionSpec as P

NORM_EPS = 1e-5
MESH = pl.DeviceIdType.MESH
N = 384
C = 128
D = 16
ROWS = N // D
BLK = 96
CPD = C // D
CHUNK = 8
NCHUNK = ROWS // CHUNK
LT = N // 128
UPDATES = 8


def sigmoid(x):
    return 0.5 * jnp.tanh(0.5 * x) + 0.5


def norm_channels(v, gamma, beta):
    mean = jnp.sum(v, axis=0, keepdims=True) * (1.0 / C)
    centered = v - mean
    variance = jnp.sum(centered * centered, axis=0, keepdims=True) * (1.0 / C)
    return centered * lax.rsqrt(variance + NORM_EPS) * gamma + beta


def kernel(z_in, m_in, gin, bin_, wp, wg, gout, bout, wo, out,
           zrow, mrow, mask, z, gate, x, q, y, ab, r, s, t, tsend, trecv,
           relay, zsend_sem, msend_sem, fsend_sem, zrecv_sem, mrecv_sem, lrecv_sem, absend_sem, abrecv_sem,
           tsend_sem, trecv_sem, osend_sem, orecv_sem):
    g = lax.axis_index("data")
    jz = lax.axis_index("dap2")
    iy = lax.axis_index("dap")
    half = jz // 2
    zl = jz % 2
    core = iy % 2
    me = iy * 4 + g * 2 + zl
    row0 = me * ROWS

    def place(n):
        k = n // 2
        dz = 1 - n % 2
        step = (k + 2 * core) % 4
        lo = 1 - k // 6
        dy = dz * (1 - step // 2) + (1 - dz) * (1 - (k % 3) // 2) * lo
        dx = dz * (((step + 1) // 2) % 2) + (1 - dz) * (((k % 3 + 1) // 2) * lo + core * dy) % 2
        dc = dz * (k // 4) + (1 - dz) * (lo * (k // 3) + (1 - lo) * (1 - k % 2))
        px = (g + dx) % 2
        pz = (zl + dz) % 2
        py = ((iy // 2 + dy) % 2) * 2 + (core + dc) % 2
        return (px, 2 * half + pz, py), py * 4 + px * 2 + pz

    def cols(j):
        return pl.ds(pl.multiple_of(j * BLK, 32), BLK)

    def block_out(q_, c, start):
        px, pz = q_ // 2, 2 * g + q_ % 2
        rows = pl.ds(c * CHUNK, CHUNK)
        src = z_in.at[pl.ds(q_ * ROWS + c * CHUNK, CHUNK)]
        into = zrow.at[rows, cols(jz), :]
        stay = px == g
        there = pz == jz

        def go(copy):
            if start:
                copy.start()
            else:
                copy.wait_send()

        @pl.when(jnp.logical_or(jnp.logical_and(stay, jnp.logical_not(there)), jnp.logical_and(jnp.logical_not(stay), there)))
        def _():
            go(pltpu.make_async_remote_copy(src, into, zsend_sem.at[q_, c], zrecv_sem.at[c],
                                            device_id=(px, pz, iy), device_id_type=MESH))

        @pl.when(jnp.logical_and(jnp.logical_not(stay), jnp.logical_not(there)))
        def _():
            go(pltpu.make_async_remote_copy(src, relay.at[q_ % 2, rows], zsend_sem.at[q_, c], lrecv_sem.at[q_ % 2, c],
                                            device_id=(px, jz, iy), device_id_type=MESH))

        if start:
            @pl.when(jnp.logical_and(stay, there))
            def _():
                pltpu.make_async_copy(src, into, zrecv_sem.at[c]).start()

    def pass_on(zq, c, start):
        rows = pl.ds(c * CHUNK, CHUNK)
        pz = 2 * (1 - g) + zq

        @pl.when(pz != jz)
        def _():
            copy = pltpu.make_async_remote_copy(relay.at[zq, rows], zrow.at[rows, cols(jz), :], fsend_sem.at[zq, c],
                                                zrecv_sem.at[c], device_id=(g, pz, iy), device_id_type=MESH)
            if start:
                got = relay.at[zq, rows]
                pltpu.make_async_copy(got, got, lrecv_sem.at[zq, c]).wait()
                copy.start()
            else:
                copy.wait_send()

    def mask_out(q_, start):
        here = jnp.logical_and(q_ // 2 == g, jz == 2 * g + q_ % 2)
        src = m_in.at[pl.ds(q_ * ROWS, ROWS)]

        @pl.when(jnp.logical_not(here))
        def _():
            copy = pltpu.make_async_remote_copy(src, mrow.at[jz], msend_sem.at[q_], mrecv_sem,
                                                device_id=(q_ // 2, 2 * g + q_ % 2, iy), device_id_type=MESH)
            if start:
                copy.start()
            else:
                copy.wait_send()

        if start:
            @pl.when(here)
            def _():
                pltpu.make_async_copy(src, mrow.at[jz], mrecv_sem).start()

    for q_ in range(4):
        mask_out(q_, True)
    for c in range(NCHUNK):
        for q_ in range(4):
            block_out(q_, c, True)
    for c in range(NCHUNK):
        for zq in range(2):
            pass_on(zq, c, True)
    pltpu.make_async_copy(mrow, mrow, mrecv_sem).wait()
    lane = lax.broadcasted_iota(jnp.int32, (128, N), 0)
    col = lax.broadcasted_iota(jnp.int32, (128, N), 1)
    total = jnp.zeros((ROWS, N), jnp.float32)
    for j in range(4):
        pick = jnp.logical_and(col == lane + j * BLK, lane < BLK).astype(jnp.float32)
        total = total + jnp.dot(mrow[j], pick, preferred_element_type=jnp.float32)
    mask[...] = total

    def project(u, p):
        for h in range(2):
            for lt in range(LT):
                v = z[2 * p + h, :, pl.ds(lt * 128, 128)].astype(jnp.float32)
                xn = norm_channels(v, gin[u], bin_[u])
                x[:, pl.ds(h * N + lt * 128, 128)] = xn.astype(jnp.bfloat16)
        q[pl.ds(0, 4 * C), :] = jnp.dot(wp[u], x[...], preferred_element_type=jnp.float32)
        q[pl.ds(4 * C, C), :] = jnp.dot(wg[u], x[...], preferred_element_type=jnp.float32)
        for h in range(2):
            cols = pl.ds(h * N, N)
            m = mask[pl.ds(2 * p + h, 1), :]
            for d in range(D):
                def part(k):
                    return q[pl.ds(k * C + d * CPD, CPD), cols]
                left = m * sigmoid(part(1)) * part(0)
                right = m * sigmoid(part(3)) * part(2)
                ab[d, 2 * p + h] = jnp.concatenate([left, right], axis=0).astype(jnp.bfloat16)
                gate[2 * p + h, pl.ds(d * CPD, CPD), :] = sigmoid(part(4))

    def finish(u, p):
        for lt in range(LT):
            tv = trecv[:, p, :, pl.ds(lt * 128, 128)].astype(jnp.float32)
            for h in range(2):
                v = tv[:, h * CPD:(h + 1) * CPD, :].reshape(C, 128)
                yn = norm_channels(v, gout[u], bout[u])
                y[:, pl.ds(h * N + lt * 128, 128)] = yn.astype(jnp.bfloat16)
        q[pl.ds(0, C), :] = jnp.dot(wo[u], y[...], preferred_element_type=jnp.float32)
        for h in range(2):
            for k in range(C // 16):
                rows = pl.ds(k * 16, 16)
                upd = gate[2 * p + h, rows, :] * q[rows, pl.ds(h * N, N)]
                z[2 * p + h, rows, :] = (z[2 * p + h, rows, :].astype(jnp.float32) + upd).astype(jnp.bfloat16)

    def send_ab(c):
        mine = pl.ds(pl.multiple_of(row0 + c * CHUNK, 8), CHUNK)
        rows = pl.ds(c * CHUNK, CHUNK)

        def to(d, _):
            dst, num = place(d)
            pltpu.make_async_remote_copy(ab.at[num, rows], r.at[mine], absend_sem, abrecv_sem.at[c],
                                         device_id=dst, device_id_type=MESH).start()
            return 0

        lax.fori_loop(0, D - 1, to, 0)
        r[mine] = ab[me, rows]

    def project_chunk(u, c):
        def one(p, _):
            project(u, c * (CHUNK // 2) + p)
            return 0

        lax.fori_loop(0, CHUNK // 2, one, 0)
        send_ab(c)

    for c in range(NCHUNK):
        got = zrow.at[pl.ds(c * CHUNK, CHUNK)]
        pltpu.make_async_copy(got, got, zrecv_sem.at[c]).wait()

        def turn_in(i, _):
            z[c * CHUNK + i] = zrow[c * CHUNK + i].T
            return 0

        lax.fori_loop(0, CHUNK, turn_in, 0)
        project_chunk(0, c)
    for q_ in range(4):
        mask_out(q_, False)
        for c in range(NCHUNK):
            block_out(q_, c, False)
    for c in range(NCHUNK):
        for zq in range(2):
            pass_on(zq, c, False)

    def block_back(j, c, start):
        here = jnp.logical_and(half == g, jz == j)
        src = zrow.at[pl.ds(c * CHUNK, CHUNK), pl.ds(j * BLK, BLK), :]
        into = out.at[pl.ds(pl.multiple_of((2 * g + zl) * ROWS + c * CHUNK, 8), CHUNK)]

        @pl.when(jnp.logical_not(here))
        def _():
            copy = pltpu.make_async_remote_copy(src, into, osend_sem.at[j, c], orecv_sem,
                                                device_id=(half, j, iy), device_id_type=MESH)
            if start:
                copy.start()
            else:
                copy.wait_send()

        if start:
            @pl.when(here)
            def _():
                pltpu.make_async_copy(src, into, orecv_sem).start()

    def update(u, _):
        for c in range(NCHUNK):
            part = r.at[pl.ds(0, (D - 1) * CHUNK)]
            pltpu.make_async_copy(part, part, abrecv_sem.at[c]).wait()

            def turn(k, _):
                rows = pl.ds(pl.multiple_of(k * ROWS + c * CHUNK, 8), CHUNK)
                for lt in range(LT):
                    v = r[rows, :, pl.ds(lt * 128, 128)].astype(jnp.float32)
                    s[:, lt, rows, :] = jnp.swapaxes(v, 0, 1)
                return 0

            lax.fori_loop(0, D, turn, 0)

        def square(c):
            return jnp.concatenate([s[c, lt] for lt in range(LT)], axis=1).astype(jnp.bfloat16)

        def contract(c, dims):
            prod = lax.dot_general(square(c), square(c + CPD), (dims, ((), ())), preferred_element_type=jnp.float32)
            for lt in range(LT):
                t[c, lt] = prod[:, lt * 128:(lt + 1) * 128]

        @pl.when(u % 2 == 0)
        def _():
            def one(c, _):
                contract(c, ((1,), (1,)))
                return 0
            lax.fori_loop(0, CPD, one, 0)

        @pl.when(u % 2 == 1)
        def _():
            def one(c, _):
                contract(c, ((0,), (0,)))
                return 0
            lax.fori_loop(0, CPD, one, 0)

        for c in range(NCHUNK):
            def give(n, _):
                dst, num = place(n)
                rows = pl.ds(pl.multiple_of(num * ROWS + c * CHUNK, 8), CHUNK)
                pairs = pl.ds(num * (ROWS // 2) + c * (CHUNK // 2), CHUNK // 2)
                into = pl.ds(c * (CHUNK // 2), CHUNK // 2)
                for lt in range(LT):
                    v = jnp.swapaxes(t[:, lt, rows, :], 0, 1)
                    tsend[pairs, :, pl.ds(lt * 128, 128)] = v.reshape(CHUNK // 2, 16, 128).astype(jnp.bfloat16)

                @pl.when(n < D - 1)
                def _():
                    pltpu.make_async_remote_copy(tsend.at[pairs], trecv.at[me, into], tsend_sem, trecv_sem.at[c],
                                                 device_id=dst, device_id_type=MESH).start()

                @pl.when(n == D - 1)
                def _():
                    trecv[me, into] = tsend[pairs]
                return 0

            lax.fori_loop(0, D, give, 0)

        for c in range(NCHUNK):
            part = tsend.at[pl.ds(0, (D - 1) * (CHUNK // 2))]
            pltpu.make_async_copy(part, part, trecv_sem.at[c]).wait()
            if c == 0:
                part = ab.at[pl.ds(0, D - 1)]
                pltpu.make_async_copy(part, part, absend_sem).wait()

            def one(p, _):
                finish(u, c * (CHUNK // 2) + p)
                return 0

            lax.fori_loop(0, CHUNK // 2, one, 0)

            @pl.when(u < UPDATES - 1)
            def _():
                project_chunk(jnp.minimum(u + 1, UPDATES - 1), c)

            @pl.when(u == UPDATES - 1)
            def _():
                def turn_out(i, _):
                    zrow[c * CHUNK + i] = z[c * CHUNK + i].T
                    return 0

                lax.fori_loop(0, CHUNK, turn_out, 0)
                for j in range(4):
                    block_back(j, c, True)
        part = tsend.at[pl.ds(0, (D - 1) * (ROWS // 2))]
        pltpu.make_async_copy(part, part, tsend_sem).wait()
        return 0

    lax.fori_loop(0, UPDATES, update, 0)

    pltpu.make_async_copy(out, out, orecv_sem).wait()
    for c in range(NCHUNK):
        for j in range(4):
            block_back(j, c, False)


def local_fn(pair_act, pair_mask, in_gamma, in_beta, w_proj, w_gate, out_gamma, out_beta, w_out):
    mask = jnp.pad(pair_mask.astype(jnp.float32), ((0, 0), (0, 128 - BLK)))

    def spread(v):
        return jnp.broadcast_to(v.reshape(UPDATES, C, 1), (UPDATES, C, 128))

    def turned(w):
        return jnp.swapaxes(w.reshape((UPDATES,) + w.shape[2:]), 1, 2)

    any_spec = pl.BlockSpec(memory_space=pl.ANY)
    vmem = pl.BlockSpec(memory_space=pltpu.VMEM)
    bf16, f32 = jnp.bfloat16, jnp.float32
    return pl.pallas_call(
        kernel,
        out_shape=jax.ShapeDtypeStruct((BLK, BLK, C), bf16),
        in_specs=[any_spec, any_spec] + [vmem] * 7,
        out_specs=any_spec,
        scratch_shapes=[
            pltpu.VMEM((ROWS, N, C), bf16),
            pltpu.VMEM((4, ROWS, 128), f32),
            pltpu.VMEM((ROWS, N), f32),
            pltpu.VMEM((ROWS, C, N), bf16),
            pltpu.VMEM((ROWS, C, N), f32),
            pltpu.VMEM((C, 2 * N), bf16),
            pltpu.VMEM((5 * C, 2 * N), f32),
            pltpu.VMEM((C, 2 * N), bf16),
            pltpu.VMEM((D, ROWS, 2 * CPD, N), bf16),
            pltpu.VMEM((N, 2 * CPD, N), bf16),
            pltpu.VMEM((2 * CPD, LT, N, 128), f32),
            pltpu.VMEM((CPD, LT, N, 128), f32),
            pltpu.VMEM((N // 2, 2 * CPD, N), bf16),
            pltpu.VMEM((D, ROWS // 2, 2 * CPD, N), bf16),
            pltpu.VMEM((2, ROWS, BLK, C), bf16),
            pltpu.SemaphoreType.DMA((4, NCHUNK)),
            pltpu.SemaphoreType.DMA((4,)),
            pltpu.SemaphoreType.DMA((2, NCHUNK)),
            pltpu.SemaphoreType.DMA((NCHUNK,)),
            pltpu.SemaphoreType.DMA,
            pltpu.SemaphoreType.DMA((2, NCHUNK)),
            pltpu.SemaphoreType.DMA,
            pltpu.SemaphoreType.DMA((NCHUNK,)),
            pltpu.SemaphoreType.DMA,
            pltpu.SemaphoreType.DMA((NCHUNK,)),
            pltpu.SemaphoreType.DMA((4, NCHUNK)),
            pltpu.SemaphoreType.DMA,
        ],
        compiler_params=pltpu.CompilerParams(has_side_effects=True, vmem_limit_bytes=60 * 1024 * 1024),
        name="triangle",
    )(pair_act, mask, spread(in_gamma), spread(in_beta), turned(w_proj), turned(w_gate),
      spread(out_gamma), spread(out_beta), turned(w_out))


def solution(mesh):
    pair_spec = P(("data", "dap"), "dap2", None)
    mask_spec = P(("data", "dap"), "dap2")
    return jax.shard_map(local_fn, mesh=mesh, in_specs=(pair_spec, mask_spec) + (P(),) * 7,
                         out_specs=pair_spec, check_vma=False)
```

```python
import functools

import jax
import jax.numpy as jnp
from jax import lax
from jax.experimental import pallas as pl
from jax.experimental.pallas import tpu as pltpu
from jax.sharding import PartitionSpec as P

NORM_EPS = 1e-5
MESH = pl.DeviceIdType.MESH
N = 384
C = 128
D = 16
ROWS = N // D
BLK = 96
CPD = C // D
CHUNK = 8
NCHUNK = ROWS // CHUNK
LT = N // 128
UPDATES = 8


def sigmoid(x):
    return 0.5 * jnp.tanh(0.5 * x) + 0.5


def norm_channels(v, gamma, beta):
    mean = jnp.sum(v, axis=0, keepdims=True) * (1.0 / C)
    centered = v - mean
    variance = jnp.sum(centered * centered, axis=0, keepdims=True) * (1.0 / C)
    return centered * lax.rsqrt(variance + NORM_EPS) * gamma + beta


def kernel(z_in, m_in, gin_in, bin_in, wp_in, wg_in, gout_in, bout_in, wo_in, out,
           wp, wg, wo, gin, bin_, gout, bout, msend, zrow, mrow, mask, z, gate, x, q, y, ab, r, s, t, tsend, trecv,
           relay, zsend_sem, msend_sem, fsend_sem, zrecv_sem, mrecv_sem, lrecv_sem, absend_sem, abrecv_sem,
           tsend_sem, trecv_sem, osend_sem, orecv_sem):
    g = lax.axis_index("data")
    jz = lax.axis_index("dap2")
    iy = lax.axis_index("dap")
    half = jz // 2
    zl = jz % 2
    core = iy % 2
    me = iy * 4 + g * 2 + zl

    def place(n):
        k = n // 2
        dz = 1 - n % 2
        step = (k + 2 * core) % 4
        lo = 1 - k // 6
        dy = dz * (1 - step // 2) + (1 - dz) * (1 - (k % 3) // 2) * lo
        dx = dz * (((step + 1) // 2) % 2) + (1 - dz) * (((k % 3 + 1) // 2) * lo + core * dy) % 2
        dc = dz * (k // 4) + (1 - dz) * (lo * (k // 3) + (1 - lo) * (1 - k % 2))
        px = (g + dx) % 2
        pz = (zl + dz) % 2
        py = ((iy // 2 + dy) % 2) * 2 + (core + dc) % 2
        return (px, 2 * half + pz, py), py * 4 + px * 2 + pz

    def cols(j):
        return pl.ds(pl.multiple_of(j * BLK, 32), BLK)

    def block_out(q_, c, start):
        px, pz = q_ // 2, 2 * g + q_ % 2
        rows = pl.ds(c * CHUNK, CHUNK)
        src = z_in.at[pl.ds(q_ * ROWS + c * CHUNK, CHUNK)]
        into = zrow.at[rows, cols(jz), :]
        stay = px == g
        there = pz == jz

        def go(copy):
            if start:
                copy.start()
            else:
                copy.wait_send()

        @pl.when(jnp.logical_or(jnp.logical_and(stay, jnp.logical_not(there)), jnp.logical_and(jnp.logical_not(stay), there)))
        def _():
            go(pltpu.make_async_remote_copy(src, into, zsend_sem.at[q_, c], zrecv_sem.at[c],
                                            device_id=(px, pz, iy), device_id_type=MESH))

        @pl.when(jnp.logical_and(jnp.logical_not(stay), jnp.logical_not(there)))
        def _():
            go(pltpu.make_async_remote_copy(src, relay.at[q_ % 2, rows], zsend_sem.at[q_, c], lrecv_sem.at[q_ % 2, c],
                                            device_id=(px, jz, iy), device_id_type=MESH))

        if start:
            @pl.when(jnp.logical_and(stay, there))
            def _():
                pltpu.make_async_copy(src, into, zrecv_sem.at[c]).start()

    def pass_on(zq, c, start):
        rows = pl.ds(c * CHUNK, CHUNK)
        pz = 2 * (1 - g) + zq

        @pl.when(pz != jz)
        def _():
            copy = pltpu.make_async_remote_copy(relay.at[zq, rows], zrow.at[rows, cols(jz), :], fsend_sem.at[zq, c],
                                                zrecv_sem.at[c], device_id=(g, pz, iy), device_id_type=MESH)
            if start:
                got = relay.at[zq, rows]
                pltpu.make_async_copy(got, got, lrecv_sem.at[zq, c]).wait()
                copy.start()
            else:
                copy.wait_send()

    def mask_out(q_, start):
        here = jnp.logical_and(q_ // 2 == g, jz == 2 * g + q_ % 2)
        rows = pl.ds(q_ * ROWS, ROWS)
        src = msend.at[rows]

        @pl.when(jnp.logical_not(here))
        def _():
            copy = pltpu.make_async_remote_copy(src, mrow.at[jz], msend_sem.at[q_], mrecv_sem,
                                                device_id=(q_ // 2, 2 * g + q_ % 2, iy), device_id_type=MESH)
            if start:
                copy.start()
            else:
                copy.wait_send()

        if start:
            @pl.when(here)
            def _():
                mrow[jz] = msend[rows]

    for c in range(NCHUNK):
        for q_ in range(4):
            block_out(q_, c, True)
    msend[...] = jnp.zeros_like(msend)
    msend[:, pl.ds(0, BLK)] = m_in[...].astype(jnp.float32)
    for q_ in range(4):
        mask_out(q_, True)

    def prepare(u, _):
        wp[u] = wp_in[u].T
        wg[u] = wg_in[u].T
        wo[u] = wo_in[u].T
        for src, dst in ((gin_in, gin), (bin_in, bin_), (gout_in, gout), (bout_in, bout)):
            dst[u] = jnp.broadcast_to(src[u // 2, pl.ds(u % 2, 1), :], (C, C)).T
        return 0

    lax.fori_loop(0, UPDATES, prepare, 0)
    for c in range(NCHUNK):
        for zq in range(2):
            pass_on(zq, c, True)
    for n_from in (3, 4):
        @pl.when((n_from == 3) == (half == g))
        def _():
            part = mrow.at[pl.ds(0, n_from)]
            pltpu.make_async_copy(part, part, mrecv_sem).wait()
    lane = lax.broadcasted_iota(jnp.int32, (128, N), 0)
    col = lax.broadcasted_iota(jnp.int32, (128, N), 1)
    natural = (col % 128) // CHUNK * ROWS + col // 128 * CHUNK + col % CHUNK
    total = jnp.zeros((ROWS, N), jnp.float32)
    for j in range(4):
        pick = jnp.logical_and(natural == lane + j * BLK, lane < BLK).astype(jnp.float32)
        total = total + jnp.dot(mrow[j], pick, preferred_element_type=jnp.float32)
    mask[...] = total

    def project(u, p):
        for h in range(2):
            for lt in range(LT):
                v = z[2 * p + h, :, pl.ds(lt * 128, 128)].astype(jnp.float32)
                xn = norm_channels(v, gin[u], bin_[u])
                x[:, pl.ds(h * N + lt * 128, 128)] = xn.astype(jnp.bfloat16)
        q[pl.ds(0, 4 * C), :] = jnp.dot(wp[u], x[...], preferred_element_type=jnp.float32)
        q[pl.ds(4 * C, C), :] = jnp.dot(wg[u], x[...], preferred_element_type=jnp.float32)
        for h in range(2):
            cols = pl.ds(h * N, N)
            m = mask[pl.ds(2 * p + h, 1), :]
            for d in range(D):
                def part(k):
                    return q[pl.ds(k * C + d * CPD, CPD), cols]
                left = m * sigmoid(part(1)) * part(0)
                right = m * sigmoid(part(3)) * part(2)
                ab[d, 2 * p + h] = jnp.concatenate([left, right], axis=0).astype(jnp.bfloat16)
                gate[2 * p + h, pl.ds(d * CPD, CPD), :] = sigmoid(part(4))

    def finish(u, p):
        for lt in range(LT):
            tv = trecv[:, p, :, pl.ds(lt * 128, 128)].astype(jnp.float32)
            for h in range(2):
                v = tv[:, h * CPD:(h + 1) * CPD, :].reshape(C, 128)
                yn = norm_channels(v, gout[u], bout[u])
                y[:, pl.ds(h * N + lt * 128, 128)] = yn.astype(jnp.bfloat16)
        q[pl.ds(0, C), :] = jnp.dot(wo[u], y[...], preferred_element_type=jnp.float32)
        for h in range(2):
            for k in range(C // 16):
                rows = pl.ds(k * 16, 16)
                upd = gate[2 * p + h, rows, :] * q[rows, pl.ds(h * N, N)]
                z[2 * p + h, rows, :] = (z[2 * p + h, rows, :].astype(jnp.float32) + upd).astype(jnp.bfloat16)

    def send_ab(c):
        mine = pl.ds(pl.multiple_of(c * 128 + me * CHUNK, 8), CHUNK)
        rows = pl.ds(c * CHUNK, CHUNK)

        def to(d, _):
            dst, num = place(d)
            pltpu.make_async_remote_copy(ab.at[num, rows], r.at[mine], absend_sem, abrecv_sem.at[c],
                                         device_id=dst, device_id_type=MESH).start()
            return 0

        lax.fori_loop(0, D - 1, to, 0)
        r[mine] = ab[me, rows]

    def project_chunk(u, c):
        def one(p, _):
            project(u, c * (CHUNK // 2) + p)
            return 0

        lax.fori_loop(0, CHUNK // 2, one, 0)
        send_ab(c)

    for c in range(NCHUNK):
        got = zrow.at[pl.ds(c * CHUNK, CHUNK)]
        pltpu.make_async_copy(got, got, zrecv_sem.at[c]).wait()

        def turn_in(i, _):
            v = zrow[c * CHUNK + i].astype(jnp.float32)
            v = jnp.concatenate([v[k * ROWS + e * CHUNK:k * ROWS + (e + 1) * CHUNK]
                                 for e in range(NCHUNK) for k in range(D)], axis=0)
            z[c * CHUNK + i] = v.T.astype(jnp.bfloat16)
            return 0

        lax.fori_loop(0, CHUNK, turn_in, 0)
        project_chunk(0, c)
    for q_ in range(4):
        mask_out(q_, False)
        for c in range(NCHUNK):
            block_out(q_, c, False)
    for c in range(NCHUNK):
        for zq in range(2):
            pass_on(zq, c, False)

    def block_back(j, c, start):
        here = jnp.logical_and(half == g, jz == j)
        src = zrow.at[pl.ds(c * CHUNK, CHUNK), pl.ds(j * BLK, BLK), :]
        into = out.at[pl.ds(pl.multiple_of((2 * g + zl) * ROWS + c * CHUNK, 8), CHUNK)]

        @pl.when(jnp.logical_not(here))
        def _():
            copy = pltpu.make_async_remote_copy(src, into, osend_sem.at[j, c], orecv_sem,
                                                device_id=(half, j, iy), device_id_type=MESH)
            if start:
                copy.start()
            else:
                copy.wait_send()

        if start:
            @pl.when(here)
            def _():
                pltpu.make_async_copy(src, into, orecv_sem).start()

    def update(u, _):
        def block(ch, c, lts=range(LT)):
            rows = pl.ds(c * 128, 128)
            return jnp.concatenate([s[ch, lt, rows, :] for lt in lts], axis=1).astype(jnp.bfloat16)

        def dot(lhs, rhs, dim):
            return lax.dot_general(lhs, rhs, (((dim,), (dim,)), ((), ())), preferred_element_type=jnp.float32)

        def outer(rows, lts):
            def one(ch, _):
                right = [block(ch + CPD, lt) for lt in lts]
                right = jnp.concatenate(right, axis=0)
                for i in rows:
                    prod = dot(block(ch, i), right, 1)
                    for n, lt in enumerate(lts):
                        t[ch, lt, pl.ds(i * 128, 128), :] = prod[:, n * 128:(n + 1) * 128]
                return 0

            @pl.when(u % 2 == 0)
            def _():
                lax.fori_loop(0, CPD, one, 0)

        def inner(rows, c):
            def one(ch, _):
                right = block(ch + CPD, c)
                for i in rows:
                    prod = dot(block(ch, c, (i,)), right, 0)
                    for lt in range(LT):
                        at = pl.ds(i * 128, 128)
                        part = prod[:, lt * 128:(lt + 1) * 128]
                        t[ch, lt, at, :] = part if c == 0 else t[ch, lt, at, :] + part
                return 0

            @pl.when(u % 2 == 1)
            def _():
                lax.fori_loop(0, CPD, one, 0)

        for c in range(NCHUNK):
            part = r.at[pl.ds(0, (D - 1) * CHUNK)]
            pltpu.make_async_copy(part, part, abrecv_sem.at[c]).wait()

            def turn(k, _):
                rows = pl.ds(pl.multiple_of(c * 128 + k * CHUNK, 8), CHUNK)
                for lt in range(LT):
                    v = r[rows, :, pl.ds(lt * 128, 128)].astype(jnp.float32)
                    s[:, lt, rows, :] = jnp.swapaxes(v, 0, 1)
                return 0

            lax.fori_loop(0, D, turn, 0)
            if c < NCHUNK - 1:
                outer(range(c), (c,))
                outer((c,), range(c + 1))
                inner(range(LT), c)

        last = NCHUNK - 1
        for c in range(NCHUNK):
            outer((c,), range(NCHUNK) if c == last else (last,))
            inner((c,), last)

            def give(n, _):
                dst, num = place(n)
                rows = pl.ds(pl.multiple_of(c * 128 + num * CHUNK, 8), CHUNK)
                pairs = pl.ds(num * (ROWS // 2) + c * (CHUNK // 2), CHUNK // 2)
                into = pl.ds(c * (CHUNK // 2), CHUNK // 2)
                for lt in range(LT):
                    v = jnp.swapaxes(t[:, lt, rows, :], 0, 1)
                    tsend[pairs, :, pl.ds(lt * 128, 128)] = v.reshape(CHUNK // 2, 16, 128).astype(jnp.bfloat16)

                @pl.when(n < D - 1)
                def _():
                    pltpu.make_async_remote_copy(tsend.at[pairs], trecv.at[me, into], tsend_sem, trecv_sem.at[c],
                                                 device_id=dst, device_id_type=MESH).start()

                @pl.when(n == D - 1)
                def _():
                    trecv[me, into] = tsend[pairs]
                return 0

            lax.fori_loop(0, D, give, 0)

        for c in range(NCHUNK):
            part = tsend.at[pl.ds(0, (D - 1) * (CHUNK // 2))]
            pltpu.make_async_copy(part, part, trecv_sem.at[c]).wait()
            if c == 0:
                part = ab.at[pl.ds(0, D - 1)]
                pltpu.make_async_copy(part, part, absend_sem).wait()

            def one(p, _):
                finish(u, c * (CHUNK // 2) + p)
                return 0

            lax.fori_loop(0, CHUNK // 2, one, 0)

            @pl.when(u < UPDATES - 1)
            def _():
                project_chunk(jnp.minimum(u + 1, UPDATES - 1), c)

            @pl.when(u == UPDATES - 1)
            def _():
                def turn_out(i, _):
                    v = z[c * CHUNK + i].astype(jnp.float32).T
                    v = jnp.concatenate([v[e * 128 + k * CHUNK:e * 128 + (k + 1) * CHUNK]
                                         for k in range(D) for e in range(NCHUNK)], axis=0)
                    zrow[c * CHUNK + i] = v.astype(jnp.bfloat16)
                    return 0

                lax.fori_loop(0, CHUNK, turn_out, 0)
                for j in range(4):
                    block_back(j, c, True)
        part = tsend.at[pl.ds(0, (D - 1) * (ROWS // 2))]
        pltpu.make_async_copy(part, part, tsend_sem).wait()
        return 0

    lax.fori_loop(0, UPDATES, update, 0)

    pltpu.make_async_copy(out, out, orecv_sem).wait()
    for c in range(NCHUNK):
        for j in range(4):
            block_back(j, c, False)


def local_fn(pair_act, pair_mask, in_gamma, in_beta, w_proj, w_gate, out_gamma, out_beta, w_out):
    def flat(w):
        return w.reshape((UPDATES,) + w.shape[2:])

    any_spec = pl.BlockSpec(memory_space=pl.ANY)
    vmem = pl.BlockSpec(memory_space=pltpu.VMEM)
    bf16, f32 = jnp.bfloat16, jnp.float32
    return pl.pallas_call(
        kernel,
        out_shape=jax.ShapeDtypeStruct((BLK, BLK, C), bf16),
        in_specs=[any_spec] + [vmem] * 8,
        out_specs=any_spec,
        scratch_shapes=[
            pltpu.VMEM((UPDATES, 4 * C, C), bf16),
            pltpu.VMEM((UPDATES, C, C), bf16),
            pltpu.VMEM((UPDATES, C, C), bf16),
            pltpu.VMEM((UPDATES, C, C), f32),
            pltpu.VMEM((UPDATES, C, C), f32),
            pltpu.VMEM((UPDATES, C, C), f32),
            pltpu.VMEM((UPDATES, C, C), f32),
            pltpu.VMEM((BLK, 128), f32),
            pltpu.VMEM((ROWS, N, C), bf16),
            pltpu.VMEM((4, ROWS, 128), f32),
            pltpu.VMEM((ROWS, N), f32),
            pltpu.VMEM((ROWS, C, N), bf16),
            pltpu.VMEM((ROWS, C, N), f32),
            pltpu.VMEM((C, 2 * N), bf16),
            pltpu.VMEM((5 * C, 2 * N), f32),
            pltpu.VMEM((C, 2 * N), bf16),
            pltpu.VMEM((D, ROWS, 2 * CPD, N), bf16),
            pltpu.VMEM((N, 2 * CPD, N), bf16),
            pltpu.VMEM((2 * CPD, LT, N, 128), f32),
            pltpu.VMEM((CPD, LT, N, 128), f32),
            pltpu.VMEM((N // 2, 2 * CPD, N), bf16),
            pltpu.VMEM((D, ROWS // 2, 2 * CPD, N), bf16),
            pltpu.VMEM((2, ROWS, BLK, C), bf16),
            pltpu.SemaphoreType.DMA((4, NCHUNK)),
            pltpu.SemaphoreType.DMA((4,)),
            pltpu.SemaphoreType.DMA((2, NCHUNK)),
            pltpu.SemaphoreType.DMA((NCHUNK,)),
            pltpu.SemaphoreType.DMA,
            pltpu.SemaphoreType.DMA((2, NCHUNK)),
            pltpu.SemaphoreType.DMA,
            pltpu.SemaphoreType.DMA((NCHUNK,)),
            pltpu.SemaphoreType.DMA,
            pltpu.SemaphoreType.DMA((NCHUNK,)),
            pltpu.SemaphoreType.DMA((4, NCHUNK)),
            pltpu.SemaphoreType.DMA,
        ],
        compiler_params=pltpu.CompilerParams(has_side_effects=True, vmem_limit_bytes=60 * 1024 * 1024),
        name="triangle",
    )(pair_act, pair_mask, in_gamma, in_beta, flat(w_proj), flat(w_gate), out_gamma, out_beta, flat(w_out))


def solution(mesh):
    pair_spec = P(("data", "dap"), "dap2", None)
    mask_spec = P(("data", "dap"), "dap2")
    return jax.shard_map(local_fn, mesh=mesh, in_specs=(pair_spec, mask_spec) + (P(),) * 7,
                         out_specs=pair_spec, check_vma=False)
```

```python
import functools

import jax
import jax.numpy as jnp
from jax import lax
from jax.experimental import pallas as pl
from jax.experimental.pallas import tpu as pltpu
from jax.sharding import PartitionSpec as P

NORM_EPS = 1e-5
MESH = pl.DeviceIdType.MESH
N = 384
C = 128
D = 16
ROWS = N // D
BLK = 96
CPD = C // D
CHUNK = 8
NCHUNK = ROWS // CHUNK
LT = N // 128
UPDATES = 8
GROUP = 2 * LT


def sigmoid(x):
    return 0.5 * jnp.tanh(0.5 * x) + 0.5


def norm_channels(v, gamma, beta):
    mean = jnp.sum(v, axis=0, keepdims=True) * (1.0 / C)
    centered = v - mean
    variance = jnp.sum(centered * centered, axis=0, keepdims=True) * (1.0 / C)
    return centered * lax.rsqrt(variance + NORM_EPS) * gamma + beta


def kernel(z_in, m_in, gin_in, bin_in, wp_in, wg_in, gout_in, bout_in, wo_in, out,
           wp, wg, wo, gin, bin_, gout, bout, msend, zrow, mrow, mask, z, gate, x, q, y, ab, r, s, t, tsend, trecv,
           relay, zsend_sem, msend_sem, fsend_sem, zrecv_sem, mrecv_sem, lrecv_sem, absend_sem, abrecv_sem,
           tsend_sem, trecv_sem, osend_sem, orecv_sem):
    g = lax.axis_index("data")
    jz = lax.axis_index("dap2")
    iy = lax.axis_index("dap")
    half = jz // 2
    zl = jz % 2
    core = iy % 2
    me = iy * 4 + g * 2 + zl

    def place(n):
        k = n // 2
        dz = 1 - n % 2
        step = (k + 2 * core) % 4
        lo = 1 - k // 6
        dy = dz * (1 - step // 2) + (1 - dz) * (1 - (k % 3) // 2) * lo
        dx = dz * (((step + 1) // 2) % 2) + (1 - dz) * (((k % 3 + 1) // 2) * lo + core * dy) % 2
        dc = dz * (k // 4) + (1 - dz) * (lo * (k // 3) + (1 - lo) * (1 - k % 2))
        px = (g + dx) % 2
        pz = (zl + dz) % 2
        py = ((iy // 2 + dy) % 2) * 2 + (core + dc) % 2
        return (px, 2 * half + pz, py), py * 4 + px * 2 + pz

    def cols(j):
        return pl.ds(pl.multiple_of(j * BLK, 32), BLK)

    def block_out(q_, c, start):
        px, pz = q_ // 2, 2 * g + q_ % 2
        rows = pl.ds(c * CHUNK, CHUNK)
        src = z_in.at[pl.ds(q_ * ROWS + c * CHUNK, CHUNK)]
        into = zrow.at[rows, cols(jz), :]
        stay = px == g
        there = pz == jz

        def go(copy):
            if start:
                copy.start()
            else:
                copy.wait_send()

        @pl.when(jnp.logical_or(jnp.logical_and(stay, jnp.logical_not(there)), jnp.logical_and(jnp.logical_not(stay), there)))
        def _():
            go(pltpu.make_async_remote_copy(src, into, zsend_sem.at[q_, c], zrecv_sem.at[c],
                                            device_id=(px, pz, iy), device_id_type=MESH))

        @pl.when(jnp.logical_and(jnp.logical_not(stay), jnp.logical_not(there)))
        def _():
            go(pltpu.make_async_remote_copy(src, relay.at[q_ % 2, rows], zsend_sem.at[q_, c], lrecv_sem.at[q_ % 2, c],
                                            device_id=(px, jz, iy), device_id_type=MESH))

        if start:
            @pl.when(jnp.logical_and(stay, there))
            def _():
                pltpu.make_async_copy(src, into, zrecv_sem.at[c]).start()

    def pass_on(zq, c, start):
        rows = pl.ds(c * CHUNK, CHUNK)
        pz = 2 * (1 - g) + zq

        @pl.when(pz != jz)
        def _():
            copy = pltpu.make_async_remote_copy(relay.at[zq, rows], zrow.at[rows, cols(jz), :], fsend_sem.at[zq, c],
                                                zrecv_sem.at[c], device_id=(g, pz, iy), device_id_type=MESH)
            if start:
                got = relay.at[zq, rows]
                pltpu.make_async_copy(got, got, lrecv_sem.at[zq, c]).wait()
                copy.start()
            else:
                copy.wait_send()

    def mask_out(q_, start):
        here = jnp.logical_and(q_ // 2 == g, jz == 2 * g + q_ % 2)
        rows = pl.ds(q_ * ROWS, ROWS)
        src = msend.at[rows]

        @pl.when(jnp.logical_not(here))
        def _():
            copy = pltpu.make_async_remote_copy(src, mrow.at[jz], msend_sem.at[q_], mrecv_sem,
                                                device_id=(q_ // 2, 2 * g + q_ % 2, iy), device_id_type=MESH)
            if start:
                copy.start()
            else:
                copy.wait_send()

        if start:
            @pl.when(here)
            def _():
                mrow[jz] = msend[rows]

    for c in range(NCHUNK):
        for q_ in range(4):
            block_out(q_, c, True)
    msend[...] = jnp.zeros_like(msend)
    msend[:, pl.ds(0, BLK)] = m_in[...].astype(jnp.float32)
    for q_ in range(4):
        mask_out(q_, True)

    def prepare(u, _):
        wp[u] = wp_in[u].T
        wg[u] = wg_in[u].T
        wo[u] = wo_in[u].T
        for src, dst in ((gin_in, gin), (bin_in, bin_), (gout_in, gout), (bout_in, bout)):
            dst[u] = jnp.broadcast_to(src[u // 2, pl.ds(u % 2, 1), :], (C, C)).T
        return 0

    lax.fori_loop(0, UPDATES, prepare, 0)
    for c in range(NCHUNK):
        for zq in range(2):
            pass_on(zq, c, True)
    for n_from in (3, 4):
        @pl.when((n_from == 3) == (half == g))
        def _():
            part = mrow.at[pl.ds(0, n_from)]
            pltpu.make_async_copy(part, part, mrecv_sem).wait()
    lane = lax.broadcasted_iota(jnp.int32, (128, N), 0)
    col = lax.broadcasted_iota(jnp.int32, (128, N), 1)
    natural = (col % 128) // CHUNK * ROWS + col // 128 * CHUNK + col % CHUNK
    total = jnp.zeros((ROWS, N), jnp.float32)
    for j in range(4):
        pick = jnp.logical_and(natural == lane + j * BLK, lane < BLK).astype(jnp.float32)
        total = total + jnp.dot(mrow[j], pick, preferred_element_type=jnp.float32)
    for i in range(ROWS):
        mask[i] = total[i:i + 1, :]

    def pieces(by_row, c, p):
        if by_row:
            return [(c * CHUNK + 2 * p + h, lt) for h in range(2) for lt in range(LT)]
        return [(p * GROUP + e, c) for e in range(GROUP)]

    def lanes(lt, n=1):
        return pl.ds(lt * 128, n * 128)

    def project(u, group):
        for e, (row, lt) in enumerate(group):
            v = z[row, :, lanes(lt)].astype(jnp.float32)
            x[:, lanes(e)] = norm_channels(v, gin[u], bin_[u]).astype(jnp.bfloat16)
        q[pl.ds(0, 4 * C), :] = jnp.dot(wp[u], x[...], preferred_element_type=jnp.float32)
        q[pl.ds(4 * C, C), :] = jnp.dot(wg[u], x[...], preferred_element_type=jnp.float32)
        for e, (row, lt) in enumerate(group):
            m = mask[row, :, lanes(lt)]

            def part(k):
                return q[pl.ds(k * C, C), lanes(e)]
            left = (m * sigmoid(part(1)) * part(0)).reshape(D, CPD, 128)
            right = (m * sigmoid(part(3)) * part(2)).reshape(D, CPD, 128)
            both = jnp.concatenate([left, right], axis=1).astype(jnp.bfloat16)
            ab[:, row // CHUNK, row % CHUNK, :, lanes(lt)] = both
            gate[row, :, lanes(lt)] = sigmoid(part(4))

    def finish(u, by_row, group):
        for e, (row, lt) in enumerate(group):
            h = e // LT if by_row else e % 2
            tv = trecv[:, row // 2, :, lanes(lt)].astype(jnp.float32)
            v = tv[:, h * CPD:(h + 1) * CPD, :].reshape(C, 128)
            y[:, lanes(e)] = norm_channels(v, gout[u], bout[u]).astype(jnp.bfloat16)
        q[pl.ds(0, C), :] = jnp.dot(wo[u], y[...], preferred_element_type=jnp.float32)
        for e, (row, lt) in enumerate(group):
            upd = gate[row, :, lanes(lt)] * q[pl.ds(0, C), lanes(e)]
            z[row, :, lanes(lt)] = (z[row, :, lanes(lt)].astype(jnp.float32) + upd).astype(jnp.bfloat16)

    def send_ab(by_row, c):
        def to(d, _):
            dst, num = place(d)
            if by_row:
                src, into = ab.at[num, c], r.at[c, me]
            else:
                src, into = ab.at[num, :, :, :, lanes(c)], r.at[:, me, :, :, lanes(c)]
            pltpu.make_async_remote_copy(src, into, absend_sem, abrecv_sem.at[c], device_id=dst, device_id_type=MESH).start()
            return 0

        lax.fori_loop(0, D - 1, to, 0)
        if by_row:
            r[c, me] = ab[me, c]
        else:
            for e in range(NCHUNK):
                r[e, me, :, :, lanes(c)] = ab[me, e, :, :, lanes(c)]

    def project_chunk(u, by_row, c):
        def one(p, _):
            project(u, pieces(by_row, c, p))
            return 0

        lax.fori_loop(0, ROWS * LT // NCHUNK // GROUP, one, 0)
        send_ab(by_row, c)

    for c in range(NCHUNK):
        got = zrow.at[pl.ds(c * CHUNK, CHUNK)]
        pltpu.make_async_copy(got, got, zrecv_sem.at[c]).wait()

        def turn_in(i, _):
            v = zrow[c * CHUNK + i].astype(jnp.float32)
            v = jnp.concatenate([v[k * ROWS + e * CHUNK:k * ROWS + (e + 1) * CHUNK]
                                 for e in range(NCHUNK) for k in range(D)], axis=0)
            z[c * CHUNK + i] = v.T.astype(jnp.bfloat16)
            return 0

        lax.fori_loop(0, CHUNK, turn_in, 0)
        project_chunk(0, True, c)
    for q_ in range(4):
        mask_out(q_, False)
        for c in range(NCHUNK):
            block_out(q_, c, False)
    for c in range(NCHUNK):
        for zq in range(2):
            pass_on(zq, c, False)

    def block_back(j, c, start):
        here = jnp.logical_and(half == g, jz == j)
        src = zrow.at[pl.ds(c * CHUNK, CHUNK), pl.ds(j * BLK, BLK), :]
        into = out.at[pl.ds(pl.multiple_of((2 * g + zl) * ROWS + c * CHUNK, 8), CHUNK)]

        @pl.when(jnp.logical_not(here))
        def _():
            copy = pltpu.make_async_remote_copy(src, into, osend_sem.at[j, c], orecv_sem,
                                                device_id=(half, j, iy), device_id_type=MESH)
            if start:
                copy.start()
            else:
                copy.wait_send()

        if start:
            @pl.when(here)
            def _():
                pltpu.make_async_copy(src, into, orecv_sem).start()

    def block(ch, i, outgoing):
        if outgoing:
            return jnp.concatenate([s[ch, lt, pl.ds(i * 128, 128), :] for lt in range(LT)], axis=1).astype(jnp.bfloat16)
        return s[ch, i].astype(jnp.bfloat16)

    def multiply(outgoing, rows, cols):
        dims = ((1,), (1,)) if outgoing else ((0,), (0,))

        def one(ch, _):
            right = jnp.concatenate([block(ch + CPD, lt, outgoing) for lt in cols], axis=0 if outgoing else 1)
            for i in rows:
                prod = lax.dot_general(block(ch, i, outgoing), right, (dims, ((), ())), preferred_element_type=jnp.float32)
                for n, lt in enumerate(cols):
                    t[ch, lt, pl.ds(i * 128, 128), :] = prod[:, n * 128:(n + 1) * 128]
            return 0

        lax.fori_loop(0, CPD, one, 0)

    def give(chunk, rows, cols):
        def to(n, _):
            dst, num = place(n)
            for i in rows:
                at = pl.ds(pl.multiple_of(i * 128 + num * CHUNK, 8), CHUNK)
                for lt in cols:
                    v = jnp.swapaxes(t[:, lt, at, :], 0, 1)
                    tsend[num, pl.ds(i * (CHUNK // 2), CHUNK // 2), :, lanes(lt)] = (
                        v.reshape(CHUNK // 2, 16, 128).astype(jnp.bfloat16))
            pairs = pl.ds(rows[0] * (CHUNK // 2), len(rows) * (CHUNK // 2))
            wide = lanes(cols[0], len(cols))

            @pl.when(n < D - 1)
            def _():
                pltpu.make_async_remote_copy(tsend.at[num, pairs, :, wide], trecv.at[me, pairs, :, wide], tsend_sem,
                                             trecv_sem.at[chunk], device_id=dst, device_id_type=MESH).start()

            @pl.when(n == D - 1)
            def _():
                trecv[me, pairs, :, wide] = tsend[num, pairs, :, wide]
            return 0

        lax.fori_loop(0, D, to, 0)

    def gather(by_row, c):
        part = r.at[c, pl.ds(0, D - 1)]
        pltpu.make_async_copy(part, part, abrecv_sem.at[c]).wait()

        def turn(k, _):
            for e in (c,) if by_row else range(NCHUNK):
                rows = pl.ds(pl.multiple_of(e * 128 + k * CHUNK, 8), CHUNK)
                for lt in range(LT) if by_row else (c,):
                    v = r[e, k, :, :, lanes(lt)].astype(jnp.float32)
                    s[:, lt, rows, :] = jnp.swapaxes(v, 0, 1)
            return 0

        lax.fori_loop(0, D, turn, 0)

    def update(u, outgoing):
        gather(outgoing, 0)
        multiply(outgoing, (0,), (0,))
        gather(outgoing, 1)
        multiply(outgoing, (0,), (1,))
        multiply(outgoing, (1,), (0, 1))
        for c in range(2):
            if outgoing:
                give(c, (0, 1), (c,))
            else:
                give(c, (c,), (0, 1))
        gather(outgoing, 2)
        for c in range(2):
            rows, cols = ((2,), (c,)) if outgoing else ((c,), (2,))
            multiply(outgoing, rows, cols)
            give(c, rows, cols)
        rows, cols = (range(NCHUNK), (2,)) if outgoing else ((2,), range(NCHUNK))
        multiply(outgoing, rows, cols)
        give(2, rows, cols)

        by_row = not outgoing
        for c in range(NCHUNK):
            part = trecv.at[pl.ds(0, D - 1), pl.ds(0, CHUNK // 2)]
            pltpu.make_async_copy(part, part, trecv_sem.at[c]).wait()
            if c == 0:
                part = ab.at[pl.ds(0, D - 1)]
                pltpu.make_async_copy(part, part, absend_sem).wait()

            def one(p, _):
                finish(u, by_row, pieces(by_row, c, p))
                return 0

            lax.fori_loop(0, ROWS * LT // NCHUNK // GROUP, one, 0)
            if outgoing:
                project_chunk(u + 1, by_row, c)
                continue

            @pl.when(u < UPDATES - 1)
            def _():
                project_chunk(jnp.minimum(u + 1, UPDATES - 1), by_row, c)

            @pl.when(u == UPDATES - 1)
            def _():
                def turn_out(i, _):
                    v = z[c * CHUNK + i].astype(jnp.float32).T
                    v = jnp.concatenate([v[e * 128 + k * CHUNK:e * 128 + (k + 1) * CHUNK]
                                         for k in range(D) for e in range(NCHUNK)], axis=0)
                    zrow[c * CHUNK + i] = v.astype(jnp.bfloat16)
                    return 0

                lax.fori_loop(0, CHUNK, turn_out, 0)
                for j in range(4):
                    block_back(j, c, True)
        part = tsend.at[pl.ds(0, D - 1)]
        pltpu.make_async_copy(part, part, tsend_sem).wait()

    def both(n, _):
        update(2 * n, True)
        update(2 * n + 1, False)
        return 0

    lax.fori_loop(0, UPDATES // 2, both, 0)

    pltpu.make_async_copy(out, out, orecv_sem).wait()
    for c in range(NCHUNK):
        for j in range(4):
            block_back(j, c, False)


def local_fn(pair_act, pair_mask, in_gamma, in_beta, w_proj, w_gate, out_gamma, out_beta, w_out):
    def flat(w):
        return w.reshape((UPDATES,) + w.shape[2:])

    any_spec = pl.BlockSpec(memory_space=pl.ANY)
    vmem = pl.BlockSpec(memory_space=pltpu.VMEM)
    bf16, f32 = jnp.bfloat16, jnp.float32
    return pl.pallas_call(
        kernel,
        out_shape=jax.ShapeDtypeStruct((BLK, BLK, C), bf16),
        in_specs=[any_spec] + [vmem] * 8,
        out_specs=any_spec,
        scratch_shapes=[
            pltpu.VMEM((UPDATES, 4 * C, C), bf16),
            pltpu.VMEM((UPDATES, C, C), bf16),
            pltpu.VMEM((UPDATES, C, C), bf16),
            pltpu.VMEM((UPDATES, C, C), f32),
            pltpu.VMEM((UPDATES, C, C), f32),
            pltpu.VMEM((UPDATES, C, C), f32),
            pltpu.VMEM((UPDATES, C, C), f32),
            pltpu.VMEM((BLK, 128), f32),
            pltpu.VMEM((ROWS, N, C), bf16),
            pltpu.VMEM((4, ROWS, 128), f32),
            pltpu.VMEM((ROWS, 1, N), f32),
            pltpu.VMEM((ROWS, C, N), bf16),
            pltpu.VMEM((ROWS, C, N), f32),
            pltpu.VMEM((C, 2 * N), bf16),
            pltpu.VMEM((5 * C, 2 * N), f32),
            pltpu.VMEM((C, 2 * N), bf16),
            pltpu.VMEM((D, NCHUNK, CHUNK, 2 * CPD, N), bf16),
            pltpu.VMEM((NCHUNK, D, CHUNK, 2 * CPD, N), bf16),
            pltpu.VMEM((2 * CPD, LT, N, 128), f32),
            pltpu.VMEM((CPD, LT, N, 128), f32),
            pltpu.VMEM((D, ROWS // 2, 2 * CPD, N), bf16),
            pltpu.VMEM((D, ROWS // 2, 2 * CPD, N), bf16),
            pltpu.VMEM((2, ROWS, BLK, C), bf16),
            pltpu.SemaphoreType.DMA((4, NCHUNK)),
            pltpu.SemaphoreType.DMA((4,)),
            pltpu.SemaphoreType.DMA((2, NCHUNK)),
            pltpu.SemaphoreType.DMA((NCHUNK,)),
            pltpu.SemaphoreType.DMA,
            pltpu.SemaphoreType.DMA((2, NCHUNK)),
            pltpu.SemaphoreType.DMA,
            pltpu.SemaphoreType.DMA((NCHUNK,)),
            pltpu.SemaphoreType.DMA,
            pltpu.SemaphoreType.DMA((NCHUNK,)),
            pltpu.SemaphoreType.DMA((4, NCHUNK)),
            pltpu.SemaphoreType.DMA,
        ],
        compiler_params=pltpu.CompilerParams(has_side_effects=True, vmem_limit_bytes=60 * 1024 * 1024),
        name="triangle",
    )(pair_act, pair_mask, in_gamma, in_beta, flat(w_proj), flat(w_gate), out_gamma, out_beta, flat(w_out))


def solution(mesh):
    pair_spec = P(("data", "dap"), "dap2", None)
    mask_spec = P(("data", "dap"), "dap2")
    return jax.shard_map(local_fn, mesh=mesh, in_specs=(pair_spec, mask_spec) + (P(),) * 7,
                         out_specs=pair_spec, check_vma=False)
```

```python
import functools

import jax
import jax.numpy as jnp
from jax import lax
from jax.experimental import pallas as pl
from jax.experimental.pallas import tpu as pltpu
from jax.sharding import PartitionSpec as P

NORM_EPS = 1e-5
MESH = pl.DeviceIdType.MESH
N = 384
C = 128
D = 16
ROWS = N // D
BLK = 96
CPD = C // D
CHUNK = 8
NCHUNK = ROWS // CHUNK
FEW = 4
NFEW = ROWS // FEW
LT = N // 128
UPDATES = 8
GROUP = 2 * LT


def sigmoid(x):
    return 0.5 * jnp.tanh(0.5 * x) + 0.5


def norm_channels(v, gamma, beta):
    mean = jnp.sum(v, axis=0, keepdims=True) * (1.0 / C)
    centered = v - mean
    variance = jnp.sum(centered * centered, axis=0, keepdims=True) * (1.0 / C)
    return centered * lax.rsqrt(variance + NORM_EPS) * gamma + beta


def kernel(z_in, m_in, gin_in, bin_in, wp_in, wg_in, gout_in, bout_in, wo_in, out,
           wp, wg, wo, gin, bin_, gout, bout, msend, zrow, mrow, mask, z, gate, x, q, y, ab, r, s, t, tsend, trecv,
           relay, zsend_sem, msend_sem, fsend_sem, zrecv_sem, mrecv_sem, lrecv_sem, absend_sem, abrecv_sem,
           tsend_sem, trecv_sem, osend_sem, orecv_sem):
    g = lax.axis_index("data")
    jz = lax.axis_index("dap2")
    iy = lax.axis_index("dap")
    half = jz // 2
    zl = jz % 2
    core = iy % 2
    me = iy * 4 + g * 2 + zl

    def place(n):
        k = n // 2
        dz = 1 - n % 2
        step = (k + 2 * core) % 4
        lo = 1 - k // 6
        dy = dz * (1 - step // 2) + (1 - dz) * (1 - (k % 3) // 2) * lo
        dx = dz * (((step + 1) // 2) % 2) + (1 - dz) * (((k % 3 + 1) // 2) * lo + core * dy) % 2
        dc = dz * (k // 4) + (1 - dz) * (lo * (k // 3) + (1 - lo) * (1 - k % 2))
        px = (g + dx) % 2
        pz = (zl + dz) % 2
        py = ((iy // 2 + dy) % 2) * 2 + (core + dc) % 2
        return (px, 2 * half + pz, py), py * 4 + px * 2 + pz

    def cols(j):
        return pl.ds(pl.multiple_of(j * BLK, 32), BLK)

    def block_out(q_, c, start):
        px, pz = q_ // 2, 2 * g + q_ % 2
        rows = pl.ds(c * FEW, FEW)
        src = z_in.at[pl.ds(q_ * ROWS + c * FEW, FEW)]
        done = zrecv_sem.at[c * FEW // CHUNK]
        into = zrow.at[rows, cols(jz), :]
        stay = px == g
        there = pz == jz

        def go(copy):
            if start:
                copy.start()
            else:
                copy.wait_send()

        @pl.when(jnp.logical_or(jnp.logical_and(stay, jnp.logical_not(there)), jnp.logical_and(jnp.logical_not(stay), there)))
        def _():
            go(pltpu.make_async_remote_copy(src, into, zsend_sem.at[q_, c], done,
                                            device_id=(px, pz, iy), device_id_type=MESH))

        @pl.when(jnp.logical_and(jnp.logical_not(stay), jnp.logical_not(there)))
        def _():
            go(pltpu.make_async_remote_copy(src, relay.at[q_ % 2, rows], zsend_sem.at[q_, c], lrecv_sem.at[q_ % 2, c],
                                            device_id=(px, jz, iy), device_id_type=MESH))

        if start:
            @pl.when(jnp.logical_and(stay, there))
            def _():
                pltpu.make_async_copy(src, into, done).start()

    def pass_on(zq, c, start):
        rows = pl.ds(c * FEW, FEW)
        pz = 2 * (1 - g) + zq

        @pl.when(pz != jz)
        def _():
            copy = pltpu.make_async_remote_copy(relay.at[zq, rows], zrow.at[rows, cols(jz), :], fsend_sem.at[zq, c],
                                                zrecv_sem.at[c * FEW // CHUNK], device_id=(g, pz, iy),
                                                device_id_type=MESH)
            if start:
                got = relay.at[zq, rows]
                pltpu.make_async_copy(got, got, lrecv_sem.at[zq, c]).wait()
                copy.start()
            else:
                copy.wait_send()

    def mask_out(q_, start):
        here = jnp.logical_and(q_ // 2 == g, jz == 2 * g + q_ % 2)
        rows = pl.ds(q_ * ROWS, ROWS)
        src = msend.at[rows]

        @pl.when(jnp.logical_not(here))
        def _():
            copy = pltpu.make_async_remote_copy(src, mrow.at[jz], msend_sem.at[q_], mrecv_sem,
                                                device_id=(q_ // 2, 2 * g + q_ % 2, iy), device_id_type=MESH)
            if start:
                copy.start()
            else:
                copy.wait_send()

        if start:
            @pl.when(here)
            def _():
                mrow[jz] = msend[rows]

    for c in range(NFEW):
        for q_ in range(4):
            block_out(q_, c, True)
    msend[...] = jnp.zeros_like(msend)
    msend[:, pl.ds(0, BLK)] = m_in[...].astype(jnp.float32)
    for q_ in range(4):
        mask_out(q_, True)

    def prepare(u, _):
        wp[u] = wp_in[u].T
        wg[u] = wg_in[u].T
        wo[u] = wo_in[u].T
        for src, dst in ((gin_in, gin), (bin_in, bin_), (gout_in, gout), (bout_in, bout)):
            dst[u] = jnp.broadcast_to(src[u // 2, pl.ds(u % 2, 1), :], (C, C)).T
        return 0

    for c in range(NFEW):
        if c > 0:
            lax.fori_loop(2 * c - 2, min(2 * c, UPDATES), prepare, 0)
        for zq in range(2):
            pass_on(zq, c, True)
    for n_from in (3, 4):
        @pl.when((n_from == 3) == (half == g))
        def _():
            part = mrow.at[pl.ds(0, n_from)]
            pltpu.make_async_copy(part, part, mrecv_sem).wait()
    lane = lax.broadcasted_iota(jnp.int32, (128, N), 0)
    col = lax.broadcasted_iota(jnp.int32, (128, N), 1)
    natural = (col % 128) // CHUNK * ROWS + col // 128 * CHUNK + col % CHUNK
    total = jnp.zeros((ROWS, N), jnp.float32)
    for j in range(4):
        pick = jnp.logical_and(natural == lane + j * BLK, lane < BLK).astype(jnp.float32)
        total = total + jnp.dot(mrow[j], pick, preferred_element_type=jnp.float32)
    for i in range(ROWS):
        mask[i] = total[i:i + 1, :]

    def pieces(by_row, c, p):
        if by_row:
            return [(c * CHUNK + 2 * p + h, lt) for h in range(2) for lt in range(LT)]
        return [(p * GROUP + e, c) for e in range(GROUP)]

    def lanes(lt, n=1):
        return pl.ds(lt * 128, n * 128)

    def project(u, group):
        for e, (row, lt) in enumerate(group):
            v = z[row, :, lanes(lt)].astype(jnp.float32)
            x[:, lanes(e)] = norm_channels(v, gin[u], bin_[u]).astype(jnp.bfloat16)
        q[pl.ds(0, 4 * C), :] = jnp.dot(wp[u], x[...], preferred_element_type=jnp.float32)
        q[pl.ds(4 * C, C), :] = jnp.dot(wg[u], x[...], preferred_element_type=jnp.float32)
        for e, (row, lt) in enumerate(group):
            m = mask[row, :, lanes(lt)]

            def part(k):
                return q[pl.ds(k * C, C), lanes(e)]
            left = (m * sigmoid(part(1)) * part(0)).reshape(D, CPD, 128)
            right = (m * sigmoid(part(3)) * part(2)).reshape(D, CPD, 128)
            both = jnp.concatenate([left, right], axis=1).astype(jnp.bfloat16)
            ab[:, row // CHUNK, row % CHUNK, :, lanes(lt)] = both
            gate[row, :, lanes(lt)] = sigmoid(part(4))

    def finish(u, by_row, group):
        for e, (row, lt) in enumerate(group):
            h = e // LT if by_row else e % 2
            tv = trecv[:, row // 2, :, lanes(lt)].astype(jnp.float32)
            v = tv[:, h * CPD:(h + 1) * CPD, :].reshape(C, 128)
            y[:, lanes(e)] = norm_channels(v, gout[u], bout[u]).astype(jnp.bfloat16)
        q[pl.ds(0, C), :] = jnp.dot(wo[u], y[...], preferred_element_type=jnp.float32)
        for e, (row, lt) in enumerate(group):
            upd = gate[row, :, lanes(lt)] * q[pl.ds(0, C), lanes(e)]
            z[row, :, lanes(lt)] = (z[row, :, lanes(lt)].astype(jnp.float32) + upd).astype(jnp.bfloat16)

    def send_ab(by_row, c):
        parts = 4 if by_row else 3

        def to(n, _):
            dst, num = place(n % (D - 1))
            e = n // (D - 1)
            if by_row:
                some = pl.ds(e * (CHUNK // parts), CHUNK // parts)
                src, into = ab.at[num, c, some], r.at[c, me, some]
            else:
                some = pl.ds(e * (NCHUNK // parts), NCHUNK // parts)
                src, into = ab.at[num, some, :, :, lanes(c)], r.at[some, me, :, :, lanes(c)]
            pltpu.make_async_remote_copy(src, into, absend_sem, abrecv_sem.at[c], device_id=dst, device_id_type=MESH).start()
            return 0

        lax.fori_loop(0, parts * (D - 1), to, 0)
        if by_row:
            r[c, me] = ab[me, c]
        else:
            for e in range(NCHUNK):
                r[e, me, :, :, lanes(c)] = ab[me, e, :, :, lanes(c)]

    def project_chunk(u, by_row, c):
        def one(p, _):
            project(u, pieces(by_row, c, p))
            return 0

        lax.fori_loop(0, ROWS * LT // NCHUNK // GROUP, one, 0)
        send_ab(by_row, c)

    for c in range(NCHUNK):
        got = zrow.at[pl.ds(c * CHUNK, CHUNK)]
        pltpu.make_async_copy(got, got, zrecv_sem.at[c]).wait()

        def turn_in(i, _):
            v = zrow[c * CHUNK + i].astype(jnp.float32)
            v = jnp.concatenate([v[k * ROWS + e * CHUNK:k * ROWS + (e + 1) * CHUNK]
                                 for e in range(NCHUNK) for k in range(D)], axis=0)
            z[c * CHUNK + i] = v.T.astype(jnp.bfloat16)
            return 0

        lax.fori_loop(0, CHUNK, turn_in, 0)
        project_chunk(0, True, c)
    for q_ in range(4):
        mask_out(q_, False)
        for c in range(NFEW):
            block_out(q_, c, False)
    for c in range(NFEW):
        for zq in range(2):
            pass_on(zq, c, False)

    def block_back(j, c, start):
        here = jnp.logical_and(half == g, jz == j)
        src = zrow.at[pl.ds(c * CHUNK, CHUNK), pl.ds(j * BLK, BLK), :]
        into = out.at[pl.ds(pl.multiple_of((2 * g + zl) * ROWS + c * CHUNK, 8), CHUNK)]

        @pl.when(jnp.logical_not(here))
        def _():
            copy = pltpu.make_async_remote_copy(src, into, osend_sem.at[j, c], orecv_sem,
                                                device_id=(half, j, iy), device_id_type=MESH)
            if start:
                copy.start()
            else:
                copy.wait_send()

        if start:
            @pl.when(here)
            def _():
                pltpu.make_async_copy(src, into, orecv_sem).start()

    def block(ch, i, outgoing):
        if outgoing:
            return jnp.concatenate([s[ch, lt, pl.ds(i * 128, 128), :] for lt in range(LT)], axis=1).astype(jnp.bfloat16)
        return s[ch, i].astype(jnp.bfloat16)

    def multiply(outgoing, rows, cols):
        dims = ((1,), (1,)) if outgoing else ((0,), (0,))

        def one(ch, _):
            right = jnp.concatenate([block(ch + CPD, lt, outgoing) for lt in cols], axis=0 if outgoing else 1)
            for i in rows:
                prod = lax.dot_general(block(ch, i, outgoing), right, (dims, ((), ())), preferred_element_type=jnp.float32)
                for n, lt in enumerate(cols):
                    t[ch, lt, pl.ds(i * 128, 128), :] = prod[:, n * 128:(n + 1) * 128]
            return 0

        lax.fori_loop(0, CPD, one, 0)

    def give(chunk, rows, cols):
        def to(n, _):
            dst, num = place(n)
            for i in rows:
                at = pl.ds(pl.multiple_of(i * 128 + num * CHUNK, 8), CHUNK)
                for lt in cols:
                    v = jnp.swapaxes(t[:, lt, at, :], 0, 1)
                    tsend[num, pl.ds(i * (CHUNK // 2), CHUNK // 2), :, lanes(lt)] = (
                        v.reshape(CHUNK // 2, 16, 128).astype(jnp.bfloat16))
            pairs = pl.ds(rows[0] * (CHUNK // 2), len(rows) * (CHUNK // 2))
            wide = lanes(cols[0], len(cols))

            @pl.when(n < D - 1)
            def _():
                pltpu.make_async_remote_copy(tsend.at[num, pairs, :, wide], trecv.at[me, pairs, :, wide], tsend_sem,
                                             trecv_sem.at[chunk], device_id=dst, device_id_type=MESH).start()

            @pl.when(n == D - 1)
            def _():
                trecv[me, pairs, :, wide] = tsend[num, pairs, :, wide]
            return 0

        lax.fori_loop(0, D, to, 0)

    def gather(by_row, c):
        part = r.at[c, pl.ds(0, D - 1)]
        pltpu.make_async_copy(part, part, abrecv_sem.at[c]).wait()

        def turn(k, _):
            for e in (c,) if by_row else range(NCHUNK):
                rows = pl.ds(pl.multiple_of(e * 128 + k * CHUNK, 8), CHUNK)
                for lt in range(LT) if by_row else (c,):
                    v = r[e, k, :, :, lanes(lt)].astype(jnp.float32)
                    s[:, lt, rows, :] = jnp.swapaxes(v, 0, 1)
            return 0

        lax.fori_loop(0, D, turn, 0)

    def update(u, outgoing):
        gather(outgoing, 0)
        multiply(outgoing, (0,), (0,))
        gather(outgoing, 1)
        multiply(outgoing, (0,), (1,))
        multiply(outgoing, (1,), (0, 1))
        for c in range(2):
            if outgoing:
                give(c, (0, 1), (c,))
            else:
                give(c, (c,), (0, 1))
        gather(outgoing, 2)
        for c in range(2):
            rows, cols = ((2,), (c,)) if outgoing else ((c,), (2,))
            multiply(outgoing, rows, cols)
            give(c, rows, cols)
        rows, cols = (range(NCHUNK), (2,)) if outgoing else ((2,), range(NCHUNK))
        multiply(outgoing, rows, cols)
        give(2, rows, cols)

        by_row = not outgoing
        for c in range(NCHUNK):
            part = trecv.at[pl.ds(0, D - 1), pl.ds(0, CHUNK // 2)]
            pltpu.make_async_copy(part, part, trecv_sem.at[c]).wait()
            if c == 0:
                part = ab.at[pl.ds(0, D - 1)]
                pltpu.make_async_copy(part, part, absend_sem).wait()

            def one(p, _):
                finish(u, by_row, pieces(by_row, c, p))
                return 0

            lax.fori_loop(0, ROWS * LT // NCHUNK // GROUP, one, 0)
            if outgoing:
                project_chunk(u + 1, by_row, c)
                continue

            @pl.when(u < UPDATES - 1)
            def _():
                project_chunk(jnp.minimum(u + 1, UPDATES - 1), by_row, c)

            @pl.when(u == UPDATES - 1)
            def _():
                def turn_out(i, _):
                    v = z[c * CHUNK + i].astype(jnp.float32).T
                    v = jnp.concatenate([v[e * 128 + k * CHUNK:e * 128 + (k + 1) * CHUNK]
                                         for k in range(D) for e in range(NCHUNK)], axis=0)
                    zrow[c * CHUNK + i] = v.astype(jnp.bfloat16)
                    return 0

                lax.fori_loop(0, CHUNK, turn_out, 0)
                for j in range(4):
                    block_back(j, c, True)
        part = tsend.at[pl.ds(0, D - 1)]
        pltpu.make_async_copy(part, part, tsend_sem).wait()

    def both(n, _):
        update(2 * n, True)
        update(2 * n + 1, False)
        return 0

    lax.fori_loop(0, UPDATES // 2, both, 0)

    pltpu.make_async_copy(out, out, orecv_sem).wait()
    for c in range(NCHUNK):
        for j in range(4):
            block_back(j, c, False)


def local_fn(pair_act, pair_mask, in_gamma, in_beta, w_proj, w_gate, out_gamma, out_beta, w_out):
    def flat(w):
        return w.reshape((UPDATES,) + w.shape[2:])

    any_spec = pl.BlockSpec(memory_space=pl.ANY)
    vmem = pl.BlockSpec(memory_space=pltpu.VMEM)
    bf16, f32 = jnp.bfloat16, jnp.float32
    return pl.pallas_call(
        kernel,
        out_shape=jax.ShapeDtypeStruct((BLK, BLK, C), bf16),
        in_specs=[any_spec] + [vmem] * 8,
        out_specs=any_spec,
        scratch_shapes=[
            pltpu.VMEM((UPDATES, 4 * C, C), bf16),
            pltpu.VMEM((UPDATES, C, C), bf16),
            pltpu.VMEM((UPDATES, C, C), bf16),
            pltpu.VMEM((UPDATES, C, C), f32),
            pltpu.VMEM((UPDATES, C, C), f32),
            pltpu.VMEM((UPDATES, C, C), f32),
            pltpu.VMEM((UPDATES, C, C), f32),
            pltpu.VMEM((BLK, 128), f32),
            pltpu.VMEM((ROWS, N, C), bf16),
            pltpu.VMEM((4, ROWS, 128), f32),
            pltpu.VMEM((ROWS, 1, N), f32),
            pltpu.VMEM((ROWS, C, N), bf16),
            pltpu.VMEM((ROWS, C, N), f32),
            pltpu.VMEM((C, 2 * N), bf16),
            pltpu.VMEM((5 * C, 2 * N), f32),
            pltpu.VMEM((C, 2 * N), bf16),
            pltpu.VMEM((D, NCHUNK, CHUNK, 2 * CPD, N), bf16),
            pltpu.VMEM((NCHUNK, D, CHUNK, 2 * CPD, N), bf16),
            pltpu.VMEM((2 * CPD, LT, N, 128), f32),
            pltpu.VMEM((CPD, LT, N, 128), f32),
            pltpu.VMEM((D, ROWS // 2, 2 * CPD, N), bf16),
            pltpu.VMEM((D, ROWS // 2, 2 * CPD, N), bf16),
            pltpu.VMEM((2, ROWS, BLK, C), bf16),
            pltpu.SemaphoreType.DMA((4, NFEW)),
            pltpu.SemaphoreType.DMA((4,)),
            pltpu.SemaphoreType.DMA((2, NFEW)),
            pltpu.SemaphoreType.DMA((NCHUNK,)),
            pltpu.SemaphoreType.DMA,
            pltpu.SemaphoreType.DMA((2, NFEW)),
            pltpu.SemaphoreType.DMA,
            pltpu.SemaphoreType.DMA((NCHUNK,)),
            pltpu.SemaphoreType.DMA,
            pltpu.SemaphoreType.DMA((NCHUNK,)),
            pltpu.SemaphoreType.DMA((4, NCHUNK)),
            pltpu.SemaphoreType.DMA,
        ],
        compiler_params=pltpu.CompilerParams(has_side_effects=True, vmem_limit_bytes=60 * 1024 * 1024),
        name="triangle",
    )(pair_act, pair_mask, in_gamma, in_beta, flat(w_proj), flat(w_gate), out_gamma, out_beta, flat(w_out))


def solution(mesh):
    pair_spec = P(("data", "dap"), "dap2", None)
    mask_spec = P(("data", "dap"), "dap2")
    return jax.shard_map(local_fn, mesh=mesh, in_specs=(pair_spec, mask_spec) + (P(),) * 7,
                         out_specs=pair_spec, check_vma=False)
```
